32 devices in a mesh: shard: 16 (over z, y, core), model: 2 (over x).
Axes of the slice: x: 2, y: 2, z: 4, core: 2. Of those that a mesh axis runs over, the one named last changes fastest.
Arguments:
- gradients: float32 [128, 128, 4096], P(None, 'shard', 'model'), may hold values from -6 to 6
- momentum: float32 [128, 128, 4096], P(None, 'shard', 'model'), may hold values from -6 to 6
- weights: float32 [128, 128, 4096], P(None, 'shard', 'model'), may hold values from -0.1875 to 0.1875
Outputs:
- new_weights: float32 [128, 128, 4096], P(None, 'shard', 'model')
- new_momentum: float32 [128, 128, 4096], P(None, 'shard', 'model')
The draws below stay inside these ranges and needn't reach their ends.
All inputs are finite; a program needn't handle non-finite values.
Results may differ from the reference program's by a relative error of at most 0.00012.
Values sent between devices are 32-bit elements; how exact they have to be, the bound alone decides.
A program may use at most 128 MiB of HBM per device.

```python
import jax
import jax.numpy as jnp
from jax import lax

SIDE = 128
WIDE = 4096
MATS = 128
ITERS = 4


def steps_of(key, dims, pieces, smallest, top_value):
    level = 1.0
    for dim, parts in pieces:
        heights = jax.random.uniform(jax.random.fold_in(jax.random.fold_in(key, 6), dim), (parts,), jnp.float32, smallest / len(pieces), top_value / len(pieces))
        level = level * jnp.repeat(jnp.exp(heights), dims[dim] // parts).reshape((-1,) + (1,) * (len(dims) - 1 - dim))
    return level


def gaussian(stream_key, dims, width, bound, split=(), kind=jnp.bfloat16):
    result = jax.random.normal(stream_key, dims, jnp.float32) * width
    if len(split) > 0:
        result = steps_of(stream_key, dims, split, -0.22, 0.18) * result
    return jnp.clip(result, min=-bound, max=bound).astype(kind)


def setup_inputs(seed: int = 0) -> dict:
    keys = jax.random.split(jax.random.key(seed), 4)
    return {
        "gradients": gaussian(keys[0], (MATS, SIDE, WIDE), 1.0, 6.0, ((1, 16), (2, 2)), jnp.float32),
        "momentum": gaussian(keys[1], (MATS, SIDE, WIDE), 1.0, 6.0, ((1, 16), (2, 2)), jnp.float32),
        "weights": gaussian(keys[2], (MATS, SIDE, WIDE), 0.03, 0.1875, ((1, 16), (2, 2)), jnp.float32),
    }


hold_rate = 0.9
learn_rate = 0.8

def reference(gradients, momentum, weights):
    new_momentum = hold_rate * momentum + gradients
    direction = hold_rate * new_momentum + gradients

    def orthogonal_one(stack):
        iterate = stack[None]
        iterate = iterate * lax.rsqrt(lax.optimization_barrier(jnp.sum(iterate * iterate, axis=(1, 2), keepdims=True)) + 1e-06)
        for step in range(ITERS):
            gram = jnp.einsum('mik,mjk->mij', iterate, iterate, precision=lax.Precision.HIGHEST)
            mixed = -4.775 * gram + 2.0315 * jnp.einsum('mij,mjk->mik', gram, gram, precision=lax.Precision.HIGHEST)
            iterate = 3.4445 * iterate + jnp.einsum('mij,mjk->mik', mixed, iterate, precision=lax.Precision.HIGHEST)
        return iterate[0]
    iterate = lax.map(orthogonal_one, direction)
    new_weights = weights - learn_rate * iterate
    return (new_weights, new_momentum)
```

```python
import functools

import jax
import jax.numpy as jnp
from jax import lax
from jax.experimental import pallas as pl
from jax.experimental.pallas import tpu as pltpu
from jax.sharding import PartitionSpec as P

ITERS = 4

hold_rate = 0.9
learn_rate = 0.8

HIGHEST = lax.Precision.HIGHEST
MESH = pl.DeviceIdType.MESH
VMEM_LIMIT = 62 * 2**20


def polynomial(gram, total, mul, eye):
    scale = lax.rsqrt(total + 1e-06)
    a = gram * scale * scale
    factor = None
    for step in range(ITERS):
        p = 3.4445 * eye - 4.775 * a + 2.0315 * mul(a, a)
        factor = p if factor is None else mul(p, factor)
        if step < ITERS - 1:
            a = mul(mul(p, a), p)
    return factor * scale


def plain(gradients, momentum, weights):
    new_momentum = hold_rate * momentum + gradients
    direction = hold_rate * new_momentum + gradients
    moved = lax.all_to_all(direction, "shard", split_axis=0, concat_axis=1, tiled=True)
    gram = lax.psum(jnp.einsum("mik,mjk->mij", moved, moved, precision=HIGHEST), "model")
    eye = jnp.eye(gram.shape[-1], dtype=jnp.float32)
    total = jnp.sum(gram * eye, axis=(1, 2), keepdims=True)

    def mul(a, b):
        return jnp.einsum("mij,mjk->mik", a, b, precision=HIGHEST)

    iterate = mul(polynomial(gram, total, mul, eye), moved)
    back = lax.all_to_all(iterate, "shard", split_axis=1, concat_axis=0, tiled=True)
    return weights - learn_rate * back, new_momentum


def kernel(
    n, models, g_hbm, m_hbm, w_hbm, nw_hbm, nm_hbm,
    gbuf, mbuf, wbuf, rows_in, rows_out, back, grams,
    g_sem, m_sem, w_sem, nm_sem, nw_sem, send1, recv1, send2, recv2, gsend, grecv,
):
    me = lax.axis_index("shard")
    mine = lax.axis_index("model")
    per, _, r, cols = gbuf.shape
    side = n * r
    tile = min(512, cols)
    half = n // 2

    def peer(k):
        return lax.rem(me // half + 1 + k // half, 2) * half + lax.rem(me + k, half)

    partners = [k for k in range(n) if k != half]

    def load(j):
        return (
            pltpu.make_async_copy(g_hbm.at[:, j], gbuf.at[j], g_sem.at[j]),
            pltpu.make_async_copy(m_hbm.at[:, j], mbuf.at[j], m_sem.at[j]),
        )

    def load_w(j):
        return pltpu.make_async_copy(w_hbm.at[:, j], wbuf.at[j], w_sem.at[j])

    def put_nm(j):
        return pltpu.make_async_copy(mbuf.at[j], nm_hbm.at[:, j], nm_sem.at[j])

    def put_nw(j):
        return pltpu.make_async_copy(wbuf.at[j], nw_hbm.at[:, j], nw_sem.at[j])

    def scatter(src, dst, send, recv, j):
        for k in partners:
            to = peer(k)
            pltpu.make_async_remote_copy(
                src_ref=src.at[j, to],
                dst_ref=dst.at[j, me],
                send_sem=send.at[j],
                recv_sem=recv.at[j],
                device_id={"shard": to},
                device_id_type=MESH,
            ).start()

    def wait_all(buf, sem, j):
        whole = buf.at[j, pl.ds(0, n - 1)]
        pltpu.make_async_copy(whole, whole, sem.at[j]).wait()

    @pl.loop(0, per)
    def _(j):
        for copy in load(j):
            copy.start()

    barrier = pltpu.get_barrier_semaphore()
    for k in partners:
        pl.semaphore_signal(barrier, inc=1, device_id={"shard": peer(k)}, device_id_type=MESH)
    for k in range(1, models):
        pl.semaphore_signal(
            barrier, inc=1, device_id={"model": lax.rem(mine + k, models)}, device_id_type=MESH
        )
    pl.semaphore_wait(barrier, n - 1 + models - 1)

    @pl.loop(0, per)
    def _(j):
        for copy in load(j):
            copy.wait()

        @pl.loop(0, n)
        def _(d):
            g = gbuf[j, d]
            moment = hold_rate * mbuf[j, d] + g
            mbuf[j, d] = moment
            gbuf[j, d] = hold_rate * moment + g

        rows_in[j, me] = gbuf[j, me]
        scatter(gbuf, rows_in, send1, recv1, j)
        put_nm(j).start()
        load_w(j).start()

    row = lax.broadcasted_iota(jnp.int32, (side, side), 0)
    col = lax.broadcasted_iota(jnp.int32, (side, side), 1)
    eye = (row == col).astype(jnp.float32)

    def mul(a, b):
        return jnp.dot(a, b, precision=HIGHEST, preferred_element_type=jnp.float32)

    def columns(j, c):
        return rows_in[j, :, :, pl.ds(pl.multiple_of(c * tile, tile), tile)].reshape(side, tile)

    @pl.loop(0, per)
    def _(j):
        wait_all(rows_in, recv1, j)
        def add(c, total):
            x = columns(j, c)
            return total + lax.dot_general(
                x, x, (((1,), (1,)), ((), ())), precision=HIGHEST,
                preferred_element_type=jnp.float32,
            )

        grams[j, mine] = lax.fori_loop(
            0, cols // tile, add, jnp.zeros((side, side), jnp.float32)
        )
        for k in range(1, models):
            pltpu.make_async_remote_copy(
                src_ref=grams.at[j, mine],
                dst_ref=grams.at[j, mine],
                send_sem=gsend.at[j],
                recv_sem=grecv.at[j],
                device_id={"model": lax.rem(mine + k, models)},
                device_id_type=MESH,
            ).start()
        if models > 1:
            wait_all_grams = grams.at[j, pl.ds(0, models - 1)]
            pltpu.make_async_copy(wait_all_grams, wait_all_grams, grecv.at[j]).wait()
        gram = grams[j, 0]
        for k in range(1, models):
            gram = gram + grams[j, k]
        total = jnp.sum(jnp.sum(gram * eye, axis=1, keepdims=True), axis=0, keepdims=True)
        factor = polynomial(gram, total, mul, eye)

        @pl.loop(0, cols // tile)
        def _(c):
            rows_out[j, :, :, pl.ds(pl.multiple_of(c * tile, tile), tile)] = mul(
                factor, columns(j, c)
            ).reshape(n, r, tile)

        back[j, me] = rows_out[j, me]
        scatter(rows_out, back, send2, recv2, j)

    @pl.loop(0, per)
    def _(j):
        load_w(j).wait()
        wait_all(back, recv2, j)

        @pl.loop(0, n)
        def _(d):
            wbuf[j, d] = wbuf[j, d] - learn_rate * back[j, d]

        put_nw(j).start()

    @pl.loop(0, per)
    def _(j):
        put_nm(j).wait()
        put_nw(j).wait()
        wait_all(gbuf, send1, j)
        wait_all(rows_out, send2, j)
        if models > 1:
            sent = grams.at[j, pl.ds(0, models - 1)]
            pltpu.make_async_copy(sent, sent, gsend.at[j]).wait()


def local(n, models, gradients, momentum, weights):
    mats, r, cols = gradients.shape
    if r % 8 or cols % 128 or mats % n or n % 2 or gradients.nbytes * 6 > 50 * 2**20:
        return plain(gradients, momentum, weights)
    per = mats // n
    side = n * r
    shape = (n, per, r, cols)
    whole = pltpu.VMEM((per, n, r, cols), jnp.float32)
    flops = 6 * per * (4 * side * side * cols + 26 * side**3)
    any_spec = pl.BlockSpec(memory_space=pl.ANY)
    new_weights, new_momentum = pl.pallas_call(
        functools.partial(kernel, n, models),
        out_shape=(jax.ShapeDtypeStruct(shape, jnp.float32),) * 2,
        in_specs=[any_spec] * 3,
        out_specs=(any_spec,) * 2,
        scratch_shapes=[whole] * 6
        + [pltpu.VMEM((per, models, side, side), jnp.float32)]
        + [pltpu.SemaphoreType.DMA((per,))] * 11,
        compiler_params=pltpu.CompilerParams(
            collective_id=0, has_side_effects=True, vmem_limit_bytes=VMEM_LIMIT
        ),
        cost_estimate=pl.CostEstimate(
            flops=flops, bytes_accessed=5 * gradients.nbytes, transcendentals=0
        ),
    )(gradients.reshape(shape), momentum.reshape(shape), weights.reshape(shape))
    return new_weights.reshape(mats, r, cols), new_momentum.reshape(mats, r, cols)


def solution(mesh):
    spec = P(None, "shard", "model")
    return jax.shard_map(
        functools.partial(local, mesh.shape["shard"], mesh.shape["model"]),
        mesh=mesh,
        in_specs=(spec,) * 3,
        out_specs=(spec,) * 2,
        check_vma=False,
    )
```

```python
import functools

import jax
import jax.numpy as jnp
from jax import lax
from jax.experimental import pallas as pl
from jax.experimental.pallas import tpu as pltpu
from jax.sharding import PartitionSpec as P

ITERS = 4

hold_rate = 0.9
learn_rate = 0.8

HIGHEST = lax.Precision.HIGHEST
MESH = pl.DeviceIdType.MESH


def polynomial(gram, total, mul, eye):
    scale = lax.rsqrt(total + 1e-06)
    a = gram * scale * scale
    factor = None
    for step in range(ITERS):
        p = 3.4445 * eye - 4.775 * a + 2.0315 * mul(a, a)
        factor = p if factor is None else mul(p, factor)
        if step < ITERS - 1:
            a = mul(mul(p, a), p)
    return factor * scale


def plain(gradients, momentum, weights):
    new_momentum = hold_rate * momentum + gradients
    direction = hold_rate * new_momentum + gradients
    moved = lax.all_to_all(direction, "shard", split_axis=0, concat_axis=1, tiled=True)
    gram = lax.psum(jnp.einsum("mik,mjk->mij", moved, moved, precision=HIGHEST), "model")
    eye = jnp.eye(gram.shape[-1], dtype=jnp.float32)
    total = jnp.sum(gram * eye, axis=(1, 2), keepdims=True)

    def mul(a, b):
        return jnp.einsum("mij,mjk->mik", a, b, precision=HIGHEST)

    iterate = mul(polynomial(gram, total, mul, eye), moved)
    back = lax.all_to_all(iterate, "shard", split_axis=1, concat_axis=0, tiled=True)
    return weights - learn_rate * back, new_momentum


def kernel(
    n, models, g_hbm, m_hbm, w_hbm, wbuf, mbuf,
    gbuf, rows_in, rows_out, back, grams,
    g_sem, m_sem, w_sem, send1, recv1, send2, recv2, gsend, grecv,
):
    me = lax.axis_index("shard")
    mine = lax.axis_index("model")
    per, _, r, cols = gbuf.shape
    side = n * r
    tile = min(512, cols)
    half = n // 2

    def peer(k):
        return lax.rem(me // half + 1 + k // half, 2) * half + lax.rem(me + k, half)

    partners = [k for pair in zip(range(half), range(half, n)) for k in pair if k != half]

    def load(j):
        return (
            pltpu.make_async_copy(g_hbm.at[:, j], gbuf.at[j], g_sem.at[j]),
            pltpu.make_async_copy(m_hbm.at[:, j], mbuf.at[:, j], m_sem.at[j]),
        )

    def load_w(j):
        return pltpu.make_async_copy(w_hbm.at[:, j], wbuf.at[:, j], w_sem.at[j])

    def scatter(src, dst, send, recv, j):
        for k in partners:
            to = peer(k)
            pltpu.make_async_remote_copy(
                src_ref=src.at[j, to],
                dst_ref=dst.at[j, me],
                send_sem=send.at[j],
                recv_sem=recv.at[j],
                device_id={"shard": to},
                device_id_type=MESH,
            ).start()

    def wait_all(buf, sem, j):
        whole = buf.at[j, pl.ds(0, n - 1)]
        pltpu.make_async_copy(whole, whole, sem.at[j]).wait()

    for copy in load(0):
        copy.start()

    barrier = pltpu.get_barrier_semaphore()
    for k in partners:
        pl.semaphore_signal(barrier, inc=1, device_id={"shard": peer(k)}, device_id_type=MESH)
    for k in range(1, models):
        pl.semaphore_signal(
            barrier, inc=1, device_id={"model": lax.rem(mine + k, models)}, device_id_type=MESH
        )
    pl.semaphore_wait(barrier, n - 1 + models - 1)

    @pl.loop(0, per)
    def _(j):
        for copy in load(j):
            copy.wait()

        @pl.when(j + 1 < per)
        def _():
            for copy in load(j + 1):
                copy.start()

        @pl.loop(0, n)
        def _(d):
            g = gbuf[j, d]
            moment = hold_rate * mbuf[d, j] + g
            mbuf[d, j] = moment
            gbuf[j, d] = hold_rate * moment + g

        rows_in[j, me] = gbuf[j, me]
        scatter(gbuf, rows_in, send1, recv1, j)
        load_w(j).start()

    row = lax.broadcasted_iota(jnp.int32, (side, side), 0)
    col = lax.broadcasted_iota(jnp.int32, (side, side), 1)
    eye = (row == col).astype(jnp.float32)

    def mul(a, b):
        return jnp.dot(a, b, precision=HIGHEST, preferred_element_type=jnp.float32)

    def columns(j, c):
        return rows_in[j, :, :, pl.ds(pl.multiple_of(c * tile, tile), tile)].reshape(side, tile)

    @pl.loop(0, per)
    def _(j):
        wait_all(rows_in, recv1, j)
        def add(c, total):
            x = columns(j, c)
            return total + lax.dot_general(
                x, x, (((1,), (1,)), ((), ())), precision=HIGHEST,
                preferred_element_type=jnp.float32,
            )

        grams[j, mine] = lax.fori_loop(
            0, cols // tile, add, jnp.zeros((side, side), jnp.float32)
        )
        for k in range(1, models):
            pltpu.make_async_remote_copy(
                src_ref=grams.at[j, mine],
                dst_ref=grams.at[j, mine],
                send_sem=gsend.at[j],
                recv_sem=grecv.at[j],
                device_id={"model": lax.rem(mine + k, models)},
                device_id_type=MESH,
            ).start()
        if models > 1:
            wait_all_grams = grams.at[j, pl.ds(0, models - 1)]
            pltpu.make_async_copy(wait_all_grams, wait_all_grams, grecv.at[j]).wait()
        gram = grams[j, 0]
        for k in range(1, models):
            gram = gram + grams[j, k]
        total = jnp.sum(jnp.sum(gram * eye, axis=1, keepdims=True), axis=0, keepdims=True)
        factor = polynomial(gram, total, mul, eye)

        @pl.loop(0, cols // tile)
        def _(c):
            rows_out[j, :, :, pl.ds(pl.multiple_of(c * tile, tile), tile)] = mul(
                factor, columns(j, c)
            ).reshape(n, r, tile)

        back[j, me] = rows_out[j, me]
        scatter(rows_out, back, send2, recv2, j)

    @pl.loop(0, per)
    def _(j):
        load_w(j).wait()
        wait_all(back, recv2, j)

        @pl.loop(0, n)
        def _(d):
            wbuf[d, j] = wbuf[d, j] - learn_rate * back[j, d]


    @pl.loop(0, per)
    def _(j):
        wait_all(gbuf, send1, j)
        wait_all(rows_out, send2, j)
        if models > 1:
            sent = grams.at[j, pl.ds(0, models - 1)]
            pltpu.make_async_copy(sent, sent, gsend.at[j]).wait()


def write(a_ref, b_ref, a_out, b_out, sems):
    copies = [
        pltpu.make_async_copy(src.at[k], dst.at[k], sems.at[i, k])
        for k in range(a_ref.shape[0])
        for i, (src, dst) in enumerate(((a_ref, a_out), (b_ref, b_out)))
    ]
    for copy in copies:
        copy.start()
    for copy in copies:
        copy.wait()


def local(n, models, gradients, momentum, weights):
    mats, r, cols = gradients.shape
    if r % 8 or cols % 128 or mats % n or n % 2 or gradients.nbytes * 6 > 50 * 2**20:
        return plain(gradients, momentum, weights)
    per = mats // n
    side = n * r
    shape = (n, per, r, cols)
    whole = pltpu.VMEM((per, n, r, cols), jnp.float32)
    flops = 6 * per * (4 * side * side * cols + 26 * side**3)
    any_spec = pl.BlockSpec(memory_space=pl.ANY)
    new_weights, new_momentum = pl.pallas_call(
        functools.partial(kernel, n, models),
        out_shape=(pltpu.VMEM(shape, jnp.float32),) * 2,
        in_specs=[any_spec] * 3,
        out_specs=(pl.BlockSpec(memory_space=pltpu.VMEM),) * 2,
        scratch_shapes=[whole] * 4
        + [pltpu.VMEM((per, models, side, side), jnp.float32)]
        + [pltpu.SemaphoreType.DMA((per,))] * 9,
        compiler_params=pltpu.CompilerParams(
            collective_id=0, has_side_effects=True, vmem_limit_bytes=4 * gradients.nbytes + 6 * 2**20
        ),
        cost_estimate=pl.CostEstimate(
            flops=flops, bytes_accessed=5 * gradients.nbytes, transcendentals=0
        ),
    )(gradients.reshape(shape), momentum.reshape(shape), weights.reshape(shape))
    new_weights, new_momentum = pl.pallas_call(
        write,
        out_shape=(jax.ShapeDtypeStruct(shape, jnp.float32),) * 2,
        in_specs=[pl.BlockSpec(memory_space=pltpu.VMEM)] * 2,
        out_specs=(any_spec,) * 2,
        scratch_shapes=[pltpu.SemaphoreType.DMA((2, n))],
        compiler_params=pltpu.CompilerParams(vmem_limit_bytes=3 * gradients.nbytes),
    )(new_weights, new_momentum)
    return new_weights.reshape(mats, r, cols), new_momentum.reshape(mats, r, cols)


def solution(mesh):
    spec = P(None, "shard", "model")
    return jax.shard_map(
        functools.partial(local, mesh.shape["shard"], mesh.shape["model"]),
        mesh=mesh,
        in_specs=(spec,) * 3,
        out_specs=(spec,) * 2,
        check_vma=False,
    )
```
